32 devices in a mesh: dp: 4 (over x, core), mp: 8 (over z, y).
Axes of the slice: x: 2, y: 2, z: 4, core: 2. Of those that a mesh axis runs over, the one named last changes fastest.
Arguments:
- tokens: bfloat16 [1280, 1792], P(('dp', 'mp')), may hold values from -6 to 6
- norm_gain: float32 [1792], replicated, may hold values from 0.5 to 1.5
- norm_bias: float32 [1792], replicated, may hold values from -3 to 3
- w_in: bfloat16 [1792, 15360], P('dp', 'mp'), may hold values from -0.125 to 0.125
- b_in: float32 [15360], P('mp'), may hold values from -3 to 3
- w_out: bfloat16 [15360, 1792], P('mp', 'dp'), may hold values from -0.046875 to 0.046875
- b_out: float32 [1792], replicated, may hold values from -3 to 3
Outputs:
- result: bfloat16 [1280, 1792], P(('dp', 'mp'))
The draws below stay inside these ranges and needn't reach their ends.
All inputs are finite; a program needn't handle non-finite values.
Results may differ from the reference program's by a relative error of at most 0.0042.
Values may be sent and summed in bfloat16 or wider, within the bound.
A program may use at most 128 MiB of HBM per device.

```python
import jax
import jax.numpy as jnp
from jax import lax

D = 1792
FF = 15360
TOK_DEV = 40
TOKENS = 1280
N_MP = 8


def block_scale(rng, dims, pieces, low, top_value):
    level, own = 1.0, jax.random.fold_in(rng, 6)
    for axis_at, shards_of in pieces:
        draws = jnp.exp(jax.random.uniform(jax.random.fold_in(own, axis_at), (shards_of,), jnp.float32, low / len(pieces), top_value / len(pieces)))
        level = level * jnp.repeat(draws, dims[axis_at] // shards_of).reshape([-1 if axis == axis_at else 1 for axis in range(len(dims))])
    return level


def scatter_about(own_key, extent, scale, limit, split=(), dtype=jnp.bfloat16):
    array = scale * jax.random.normal(own_key, extent, jnp.float32)
    if split:
        array = array * block_scale(own_key, extent, split, -0.22, 0.18)
    return jnp.clip(array, -limit, limit).astype(dtype)


def setup_inputs(seed: int = 0) -> dict:
    streams_of = jax.random.split(jax.random.key(seed), 8)
    return {
        "tokens": scatter_about(streams_of[0], (TOKENS, D), 1.0, 6.0, ((0, 32),)),
        "norm_gain": jnp.clip(jax.random.uniform(streams_of[1], (D,), jnp.float32, 0.5, 1.5), 0.5, 1.5),
        "norm_bias": scatter_about(streams_of[2], (D,), 0.5, 3.0, (), jnp.float32),
        "w_in": scatter_about(streams_of[3], (D, FF), D ** -0.5, 0.125, ((0, 4), (1, 8))),
        "b_in": scatter_about(streams_of[4], (FF,), 0.5, 3.0, ((0, 8),), jnp.float32),
        "w_out": scatter_about(streams_of[5], (FF, D), FF ** -0.5, 0.046875, ((0, 8), (1, 4))),
        "b_out": scatter_about(streams_of[6], (D,), 0.5, 3.0, (), jnp.float32),
    }


def block_rows(rows, norm_gain, norm_bias, w_in, b_in, w_out, b_out):
    values = rows.astype(jnp.float32)
    center = lax.optimization_barrier(jnp.mean(values, axis=1, keepdims=True))
    spread = lax.optimization_barrier(jnp.mean((values - center) ** 2, axis=1, keepdims=True))
    normed = ((values - center) / jnp.sqrt(spread + 1e-06) * norm_gain + norm_bias).astype(jnp.bfloat16)
    pre = jnp.dot(normed, w_in, preferred_element_type=jnp.float32) + b_in
    hidden = jax.nn.gelu(pre, approximate=False).astype(jnp.bfloat16)
    summed = jnp.dot(hidden, w_out, preferred_element_type=jnp.float32)
    return (values + summed + b_out).astype(jnp.bfloat16)

def reference(tokens, norm_gain, norm_bias, w_in, b_in, w_out, b_out):
    group = TOK_DEV * N_MP
    blocks = tokens.reshape(TOKENS // group, group, D)
    done = lax.map(lambda rows: block_rows(rows, norm_gain, norm_bias, w_in, b_in, w_out, b_out), blocks)
    return done.reshape(TOKENS, D)
```

```python
import functools

import jax
import jax.numpy as jnp
from jax import lax
from jax.experimental import pallas as pl
from jax.experimental.pallas import tpu as pltpu
from jax.sharding import PartitionSpec as P

MESH = pl.DeviceIdType.MESH
LANES = 128
VMEM_GRANT = 60 * 2**20


def flip(index, mask, size):
    out, bit = index, 1
    while bit < size:
        if mask & bit:
            out = out + bit - 2 * bit * (lax.rem(lax.div(index, bit), 2))
        bit *= 2
    return out


def column_chunks(depth):
    full, rest = depth // LANES, depth % LANES
    if rest:
        return [(t, t + full + 1) for t in range(full)] + [(full,)]
    return [(t, t + full) for t in range(full)]


def gelu(pre):
    return 0.5 * pre * (1.0 + lax.erf(pre * (0.5**0.5)))


def kernel(
    lines, tokens, gain, bias, w_in, b_in, w_out, b_out, out,
    vec, tok, win, wout, normed, hidden, part, own, from_y, sums, from_z, to_x, kept, from_x,
    tok_sem, win_sem, wout_sem, near_sem, y_sem, z_sem, x_sem, local_sem, send_sem,
):
    dp, mp = lax.axis_index("dp"), lax.axis_index("mp")
    x, core = lax.div(dp, 2), lax.rem(dp, 2)
    z, y = lax.div(mp, 2), lax.rem(mp, 2)
    ox, oy = 1 - x, 1 - y
    rows, dim = tokens.shape
    depth, units = w_in.shape
    half = units // 2
    start = half // LANES * LANES
    width = units - start
    tile = 2 * LANES if width % (2 * LANES) == 0 else LANES
    tiles = width // tile
    last = lines - 1
    side_columns = 2 * depth
    chunks = column_chunks(depth)
    per_side = len(chunks)
    full, rest = depth // LANES, depth % LANES
    pair_rows = 2 * rows

    x_dev = (2 * ox + core, mp)
    core_dev = (2 * x + 1 - core, mp)
    y_dev = (dp, 2 * z + oy)
    up_dev, down_dev = (dp, 2 * (z + 1) + y), (dp, 2 * (z - 1) + y)
    z_at = [flip(z, k, lines) for k in range(lines)]
    z_dev = [(dp, 2 * z_at[k] + y) for k in range(lines)]
    has_up, has_down = z < last, z > 0

    sends = []

    def send(src, dst, sem, device, when=None):
        copy = pltpu.make_async_remote_copy(
            src_ref=src, dst_ref=dst, send_sem=send_sem.at[len(sends)], recv_sem=sem,
            device_id=device, device_id_type=MESH,
        )
        sends.append((copy, when))
        if when is None:
            copy.start()
        else:
            pl.when(when)(copy.start)

    def arrive(dst, sem):
        pltpu.make_async_remote_copy(
            src_ref=dst, dst_ref=dst, send_sem=send_sem.at[0], recv_sem=sem,
            device_id=x_dev, device_id_type=MESH,
        ).wait_recv()

    def local(src, dst, at):
        copy = pltpu.make_async_copy(src, dst, local_sem.at[at])
        copy.start()
        return copy

    def block(r, zz, side):
        return tok.at[r, zz, side], tok_sem.at[r, zz, side]

    def own_columns(weight):
        return weight.at[:, pl.ds(pl.multiple_of(x * start, LANES), width)]

    def rows_of(weight, owner):
        return weight.at[pl.ds(pl.multiple_of(owner * depth, 16), depth), :]

    def in_tile(weight, owner, n):
        return weight.at[pl.ds(pl.multiple_of(owner * depth, 16), depth), pl.ds(n * tile, tile)]

    def out_rows(owner_core, m):
        if rest and m == full:
            return pl.multiple_of((1 - owner_core) * full * LANES, 16), rest
        return pl.multiple_of(owner_core * rest + m * LANES, 16), LANES

    def out_chunk(weight, owner, owner_core, m):
        at, size = out_rows(owner_core, m)
        return weight.at[pl.ds(pl.multiple_of(owner * depth + at, 16), size), :]

    small = [
        local(ref, vec.at[i, pl.ds(0, ref.shape[0])], i)
        for i, ref in enumerate((gain, bias, b_in, b_out))
    ]
    copies = [
        local(tokens, tok.at[0, z, 0], 4),
        local(own_columns(w_in), rows_of(win, dp), 5),
        local(own_columns(w_out), rows_of(wout, dp), 6),
    ]

    barrier = pltpu.get_barrier_semaphore()
    for partner in (x_dev, core_dev, y_dev):
        pl.semaphore_signal(barrier, inc=1, device_id=partner, device_id_type=MESH)
    for partner, exists in ((up_dev, has_up), (down_dev, has_down)):
        pl.when(exists)(
            functools.partial(
                pl.semaphore_signal, barrier, inc=1, device_id=partner, device_id_type=MESH
            )
        )
    pl.semaphore_wait(barrier, 3 + has_up.astype(jnp.int32) + has_down.astype(jnp.int32))

    copies[0].wait()
    mine = tok.at[0, z, 0]
    send(mine, tok.at[0, z, 1], tok_sem.at[0, z, 1], x_dev)
    send(mine, mine, tok_sem.at[0, z, 0], up_dev, has_up)
    send(mine, mine, tok_sem.at[0, z, 0], down_dev, has_down)
    send(mine, tok.at[1, z, 0], tok_sem.at[1, z, 0], y_dev)
    far, near, across = 2 * ox + core, 2 * x + 1 - core, 2 * ox + 1 - core
    for n in range(tiles):
        at = pl.ds(pl.multiple_of(ox * start + n * tile, LANES), tile)
        send(w_in.at[:, at], in_tile(win, dp, n), win_sem.at[n, dp], x_dev)
    for m in range(per_side):
        at, size = out_rows(core, m)
        columns = pl.ds(pl.multiple_of(ox * start, LANES), width)
        send(w_out.at[pl.ds(at, size), columns], out_chunk(wout, dp, core, m), wout_sem.at[m, dp], x_dev)
    send(own_columns(w_in), rows_of(win, dp), near_sem.at[0], core_dev)
    send(own_columns(w_out), rows_of(wout, dp), near_sem.at[1], core_dev)

    def forward(zz, side, up, exists=None):
        def go():
            arrive(*block(0, zz, side))

        if exists is None:
            go()
        else:
            pl.when(exists)(go)
        ref, sem = block(0, zz, side)
        further = has_up if up else has_down
        along = further if exists is None else jnp.logical_and(exists, further)
        send(ref, ref, sem, up_dev if up else down_dev, along)
        ends = 0 if up else last
        cross = exists
        if side:
            cross = jnp.logical_and(exists, zz != ends)
        send(ref, tok.at[1, zz, side], tok_sem.at[1, zz, side], y_dev, cross)

    def from_line(d, side):
        forward(z - d, side, True, z >= d)
        forward(z + d, side, False, z + d <= last)

    def normalise(r, k):
        pair = jnp.concatenate(
            [tok[r, z_at[k], 0].astype(jnp.float32), tok[r, z_at[k], 1].astype(jnp.float32)], axis=0
        )
        center = jnp.mean(pair, axis=1, keepdims=True)
        spread = jnp.mean((pair - center) ** 2, axis=1, keepdims=True)
        value = (pair - center) / jnp.sqrt(spread + 1e-06) * vec[0:1, :dim] + vec[1:2, :dim]
        normed[r, pl.ds(k * pair_rows, pair_rows), :] = value.astype(normed.dtype)

    def arrive_over_y(k):
        zz = z_at[k]
        arrive(*block(1, zz, 0))
        arrive(*block(1, zz, 1))
        ref, sem = block(1, zz, 1)
        send(ref, ref, sem, up_dev, jnp.logical_and(zz == 0, has_up))
        send(ref, ref, sem, down_dev, jnp.logical_and(zz == last, has_down))

    def activate(lhs, n):
        at = pl.ds(n * tile, tile)
        pre = jnp.dot(lhs, win[:, at], preferred_element_type=jnp.float32)
        first = pl.multiple_of(x * start + n * tile, LANES)
        pre = pre + vec[2:3, pl.ds(first, tile)]
        unit = first + lax.broadcasted_iota(jnp.int32, pre.shape, 1)
        keep = (unit >= x * half) & (unit < (x + 1) * half)
        return jnp.where(keep, gelu(pre), 0.0).astype(hidden.dtype)

    def first_pair(k, n):
        at = pl.ds(k * pair_rows, pair_rows)
        value = activate(jnp.concatenate([normed[0, at, :], normed[1, at, :]], axis=0), n)
        hidden[0, at, pl.ds(n * tile, tile)] = value[:pair_rows]
        hidden[1, at, pl.ds(n * tile, tile)] = value[pair_rows:]

    def first_all(n):
        everyone = normed[...].reshape(2 * lines * pair_rows, dim)
        value = activate(everyone, n)
        hidden[:, :, pl.ds(n * tile, tile)] = value.reshape(2, lines * pair_rows, tile)

    def tile_forward(n):
        arrive(in_tile(win, far, n), win_sem.at[n, far])
        send(in_tile(win, far, n), in_tile(win, far, n), win_sem.at[n, far], core_dev)

    def tile_ready(n):
        arrive(in_tile(win, across, n), win_sem.at[n, across])

    def weights(side, m):
        return jnp.concatenate(
            [
                wout[pl.ds(pl.multiple_of(side * side_columns + t * LANES, LANES), LANES), :]
                for t in chunks[m]
            ],
            axis=0,
        )

    def cols(m):
        return pl.ds(0, len(chunks[m]) * LANES)

    def product(q, m):
        j = q * per_side + m
        weight = weights(x if q == 0 else ox, m)

        def second(r):
            value = lax.dot_general(
                hidden[r], weight, (((1,), (1,)), ((), ())), preferred_element_type=jnp.float32
            )
            return value.reshape(lines, pair_rows, -1)

        part[j, :, :, cols(m)] = second(1).astype(part.dtype)
        send(part.at[j, :, :, cols(m)], from_y.at[j, :, :, cols(m)], y_sem.at[j], y_dev)
        own[j, :, :, cols(m)] = second(0)

    def along_z(q, m):
        j, c = q * per_side + m, cols(m)
        arrive(from_y.at[j, :, :, c], y_sem.at[j])
        for k in list(range(lines - 1, 0, -1)) + [0]:
            total = own[j, k, :, c] + from_y[j, k, :, c].astype(jnp.float32)
            if k:
                sums[j, k, :, c] = total.astype(sums.dtype)
                send(sums.at[j, k, :, c], from_z.at[j, k, :, c], z_sem.at[j, k], z_dev[k])
            else:
                own[j, 0, :, c] = total

    def along_x(q, m):
        j, c = q * per_side + m, cols(m)
        theirs = (1 - q) * per_side + m
        total = own[j, 0, :, c]
        for k in range(1, lines):
            arrive(from_z.at[j, k, :, c], z_sem.at[j, k])
            total = total + from_z[j, k, :, c].astype(jnp.float32)
        kept[j, :, c] = total[:rows]
        to_x[j, :, c] = total[rows:].astype(to_x.dtype)
        send(to_x.at[j, :, c], from_x.at[theirs, :, c], x_sem.at[theirs], x_dev)

    def finish(q, m):
        j, c = q * per_side + m, cols(m)
        side = x if q == 0 else ox
        arrive(from_x.at[j, :, c], x_sem.at[j])
        total = kept[j, :, c] + from_x[j, :, c].astype(jnp.float32)
        for i, t in enumerate(chunks[m]):
            at = pl.ds(pl.multiple_of(side * side_columns + t * LANES, LANES), LANES)
            value = tok[0, z, 0, :, at].astype(jnp.float32) + total[:, i * LANES:(i + 1) * LANES]
            out[:, at] = (value + vec[3:4, at]).astype(out.dtype)

    def own_block():
        ref, sem = block(0, z, 1)
        arrive(ref, sem)
        send(ref, ref, sem, up_dev, has_up)
        send(ref, ref, sem, down_dev, has_down)
        send(ref, tok.at[1, z, 1], tok_sem.at[1, z, 1], y_dev)

    def out_forward(m):
        arrive(out_chunk(wout, far, core, m), wout_sem.at[m, far])
        send(out_chunk(wout, far, core, m), out_chunk(wout, far, core, m), wout_sem.at[m, far], core_dev)

    def out_ready(m):
        arrive(out_chunk(wout, across, 1 - core, m), wout_sem.at[m, across])

    own_block()
    from_line(1, 0)
    for copy in small:
        copy.wait()
    normalise(0, 0)
    from_line(1, 1)
    arrive_over_y(0)
    done, known, ready = set(), [0], 0

    def catch_up():
        for k in known:
            for n in range(ready):
                if (k, n) not in done:
                    first_pair(k, n)
                    done.add((k, n))

    for d in range(1, lines):
        n = d - 1
        if n < tiles - 1:
            tile_forward(n)
        if d == 1:
            normalise(1, 0)
            copies[1].wait()
            arrive(rows_of(win, near), near_sem.at[0])
        if d + 1 < lines:
            from_line(d + 1, 0)
        if n < tiles - 1:
            tile_ready(n)
            ready = n + 1
        normalise(0, d)
        catch_up()
        if d + 1 < lines:
            from_line(d + 1, 1)
        if d < last:
            arrive_over_y(d)
            normalise(1, d)
            known.append(d)
    for n in range(ready, tiles - 1):
        tile_forward(n)
        tile_ready(n)
    ready = tiles - 1
    catch_up()
    tile_forward(tiles - 1)
    arrive_over_y(last)
    normalise(1, last)
    known.append(last)
    catch_up()
    tile_ready(tiles - 1)
    first_all(tiles - 1)

    copies[2].wait()
    arrive(rows_of(wout, near), near_sem.at[1])
    order = [(q, m) for q in range(2) for m in range(per_side)]
    n = len(order)
    for m in range(per_side):
        product(0, m)
    summed = crossed = 0
    for m in range(per_side):
        out_forward(m)
        along_z(*order[summed])
        summed += 1
        if m > 1:
            along_x(*order[crossed])
            crossed += 1
        out_ready(m)
        product(1, m)
    while crossed < n:
        if summed < n:
            along_z(*order[summed])
            summed += 1
        along_x(*order[crossed])
        crossed += 1
    for q, m in [(q, m) for m in range(per_side) for q in range(2)]:
        finish(q, m)
    for copy, when in sends:
        if when is None:
            copy.wait_send()
        else:
            pl.when(when)(copy.wait_send)


def fused(mp, tokens, gain, bias, w_in, b_in, w_out, b_out):
    rows, dim = tokens.shape
    depth, units = w_in.shape
    lines = mp // 2
    width = units - units // 2 // LANES * LANES
    chunks = column_chunks(depth)
    n, cols = 2 * len(chunks), max(len(c) for c in chunks) * LANES
    tiles = width // LANES
    bf16, f32, dma = jnp.bfloat16, jnp.float32, pltpu.SemaphoreType.DMA
    hbm = pl.BlockSpec(memory_space=pl.ANY)
    n_sends = 16 + 8 * lines + 2 * tiles + 2 * n + n * (lines + 1)
    return pl.pallas_call(
        functools.partial(kernel, lines),
        out_shape=jax.ShapeDtypeStruct((rows, dim), bf16),
        in_specs=[hbm] * 7,
        out_specs=pl.BlockSpec(memory_space=pltpu.VMEM),
        scratch_shapes=[
            pltpu.VMEM((4, max(dim, units)), f32),
            pltpu.VMEM((2, lines, 2, rows, dim), bf16),
            pltpu.VMEM((dim, width), bf16),
            pltpu.VMEM((dim, width), bf16),
            pltpu.VMEM((2, lines * 2 * rows, dim), bf16),
            pltpu.VMEM((2, lines * 2 * rows, width), bf16),
            pltpu.VMEM((n, lines, 2 * rows, cols), bf16),
            pltpu.VMEM((n, lines, 2 * rows, cols), f32),
            pltpu.VMEM((n, lines, 2 * rows, cols), bf16),
            pltpu.VMEM((n, lines, 2 * rows, cols), bf16),
            pltpu.VMEM((n, lines, 2 * rows, cols), bf16),
            pltpu.VMEM((n, rows, cols), bf16),
            pltpu.VMEM((n, rows, cols), f32),
            pltpu.VMEM((n, rows, cols), bf16),
            dma((2, lines, 2)),
            dma((tiles, 4)),
            dma((len(chunks), 4)),
            dma((2,)),
            dma((n,)),
            dma((n, lines)),
            dma((n,)),
            dma((7,)),
            dma((n_sends,)),
        ],
        compiler_params=pltpu.CompilerParams(
            collective_id=0, has_side_effects=True, vmem_limit_bytes=VMEM_GRANT
        ),
    )(tokens, gain, bias, w_in, b_in, w_out.T, b_out)


def gathered(tokens, norm_gain, norm_bias, w_in, b_in, w_out, b_out):
    values = tokens.astype(jnp.float32)
    center = jnp.mean(values, axis=1, keepdims=True)
    spread = jnp.mean((values - center) ** 2, axis=1, keepdims=True)
    normed = ((values - center) / jnp.sqrt(spread + 1e-06) * norm_gain + norm_bias).astype(
        jnp.bfloat16
    )
    w_in_full = lax.all_gather(w_in, "dp", axis=0, tiled=True)
    everyone = lax.all_gather(normed, "mp", axis=0, tiled=True)
    pre = jnp.dot(everyone, w_in_full, preferred_element_type=jnp.float32) + b_in
    hidden = jax.nn.gelu(pre, approximate=False).astype(jnp.bfloat16)
    w_out_full = lax.all_gather(w_out, "dp", axis=1, tiled=True)
    summed = lax.psum_scatter(
        jnp.dot(hidden, w_out_full, preferred_element_type=jnp.float32),
        "mp",
        scatter_dimension=0,
        tiled=True,
    )
    return (values + summed + b_out).astype(jnp.bfloat16)


def on_device(dp, mp, tokens, norm_gain, norm_bias, w_in, b_in, w_out, b_out):
    rows, (depth, units) = tokens.shape[0], w_in.shape
    fits = (
        dp == 4
        and mp % 2 == 0
        and mp & (mp - 1) == 0
        and units % LANES == 0
        and depth % 16 == 0
        and 2 * depth % LANES == 0
        and 2 * (depth % LANES) in (0, LANES)
        and mp >= 4
        and rows % 8 == 0
        and mp * 2 * rows * (2 * depth) * 2 * 24 < VMEM_GRANT
    )
    if fits:
        return fused(mp, tokens, norm_gain, norm_bias, w_in, b_in, w_out, b_out)
    return gathered(tokens, norm_gain, norm_bias, w_in, b_in, w_out, b_out)


def solution(mesh):
    placed = (P(("dp", "mp"), None), P(), P(), P("dp", "mp"), P("mp"), P("mp", "dp"), P())
    return jax.shard_map(
        functools.partial(on_device, mesh.shape["dp"], mesh.shape["mp"]),
        mesh=mesh,
        in_specs=placed,
        out_specs=P(("dp", "mp"), None),
        check_vma=False,
    )
```
